32 devices in a mesh: inst: 4 (over x, core), blk: 8 (over z, y).
Axes of the slice: x: 2, y: 2, z: 4, core: 2. Of those that a mesh axis runs over, the one named last changes fastest.
Arguments:
- state: float32 [16, 5, 16, 64, 256], P('inst', None, None, 'blk'), may hold values from -0.53 to 3.9, as said below
- multiples: int32 [7], replicated, may hold values from 1 to 4
Outputs:
- state_change: float32 [16, 5, 16, 64, 256], P('inst', None, None, 'blk')
The draws below stay inside these ranges and needn't reach their ends.
Inputs may be any that keep to these rules, and one draw needn't show every extreme that they name: `state`: density and pressure lie in 0.7 to 1.3, the axial velocity in 0.2 to 0.8 and the other two velocity components in -0.4 to 0.4; the last variable is the total energy p / 0.4 + rho (u u + v v + w w) / 2.
All inputs are finite; a program needn't handle non-finite values.
Results may differ from the reference program's by a relative error of at most 0.0003.
Values sent between devices are 32-bit elements; how exact they have to be, the bound alone decides.
No kernel may reach another device: no remote copies, remote signals or barrier semaphores. Data moves between devices by JAX's collectives and lax.ppermute only.
A program may use at most 128 MiB of HBM per device.

```python
import math
import jax
import jax.numpy as jnp
from jax import lax

NT = 16
HARM = 7
NX = 16
NZ = 256
NY = 64


def draw_state(key, part):
    subkeys = jax.random.split(key, 5)
    layout = (NT, NX, NY, NZ)
    density = jax.random.uniform(subkeys[0], layout, jnp.float32, 0.7, 1.3)
    pressure = jax.random.uniform(subkeys[1], layout, jnp.float32, 0.7, 1.3)
    axial_speed = jax.random.uniform(subkeys[2], layout, jnp.float32, 0.2, 0.8)
    swirl_speed = jax.random.uniform(subkeys[3], layout, jnp.float32, -0.4, 0.4)
    radial_speed = jax.random.uniform(subkeys[4], layout, jnp.float32, -0.4, 0.4)
    energy = pressure / 0.4 + 0.5 * density * (axial_speed * axial_speed + swirl_speed * swirl_speed + radial_speed * radial_speed)
    return jnp.stack([density, density * axial_speed, density * swirl_speed, density * radial_speed, energy], axis=1)


def with_ends(values, stream_key, smallest, top_value):
    spot = [jax.random.randint(jax.random.fold_in(stream_key, axis), (), 0, length) for axis, length in enumerate(values.shape)]
    longest = values.shape.index(max(values.shape))
    neighbour = spot[:longest] + [(spot[longest] + 1) % values.shape[longest]] + spot[longest + 1:]
    return values.at[tuple(spot)].set(smallest).at[tuple(neighbour)].set(top_value)


def setup_inputs(seed: int = 0) -> dict:
    seeds = jax.random.split(jax.random.key(seed), 3)
    return {
        "state": draw_state(jax.random.fold_in(seeds[2], 71), 0),
        "multiples": with_ends(jax.random.randint(seeds[1], (HARM,), 1, 5), jax.random.fold_in(seeds[1], 1), 1, 4).astype(jnp.int32),
    }


heat_ratio = 1.4
segment_step = 0.05
smooth_weight = 0.5
base_rate = 0.5
diagonal_weight = 3.0

def limited(lower, upper):
    return jnp.maximum(0.0, jnp.minimum(lower, upper)) + jnp.minimum(0.0, jnp.maximum(lower, upper))

def take_part(array_in, offset, amount, along):
    return lax.slice_in_dim(array_in, offset, offset + amount, axis=along)

def primitive(conserved):
    density = conserved[:, 0]
    velocity = [conserved[:, 1] / density, conserved[:, 2] / density, conserved[:, 3] / density]
    kinetic = 0.5 * density * (velocity[0] * velocity[0] + velocity[1] * velocity[1] + velocity[2] * velocity[2])
    pressure = (heat_ratio - 1.0) * (conserved[:, 4] - kinetic)
    return [density] + velocity + [pressure]

def physical(states, normal):
    density = states[0]
    pressure = states[4]
    velocity = states[1:4]
    normal_speed = velocity[normal]
    energy = pressure / (heat_ratio - 1.0) + 0.5 * density * (velocity[0] * velocity[0] + velocity[1] * velocity[1] + velocity[2] * velocity[2])
    conserved = [density, density * velocity[0], density * velocity[1], density * velocity[2], energy]
    flux = [density * normal_speed]
    for member in range(3):
        momentum = density * normal_speed * velocity[member]
        if member == normal:
            momentum = momentum + pressure
        flux.append(momentum)
    flux.append((energy + pressure) * normal_speed)
    wave_speed = jnp.abs(normal_speed) + jnp.sqrt(heat_ratio * pressure / density)
    return (flux, conserved, wave_speed)

def divergence(states, along, normal):
    extent = states[0].shape[along]
    interior = extent - 4
    left_side = []
    right_side = []
    for component in states:
        differences = take_part(component, 1, extent - 1, along) - take_part(component, 0, extent - 1, along)
        slopes = limited(take_part(differences, 0, interior + 2, along), take_part(differences, 1, interior + 2, along))
        centres = take_part(component, 1, interior + 2, along)
        left_side.append(take_part(centres, 0, interior + 1, along) + 0.5 * take_part(slopes, 0, interior + 1, along))
        right_side.append(take_part(centres, 1, interior + 1, along) - 0.5 * take_part(slopes, 1, interior + 1, along))
    left_flux, left_cons, left_speed = physical(left_side, normal)
    right_flux, right_cons, right_speed = physical(right_side, normal)
    wave_speed = jnp.maximum(left_speed, right_speed)
    result = []
    for member in range(5):
        face_flux = 0.5 * (left_flux[member] + right_flux[member]) - 0.5 * wave_speed * (right_cons[member] - left_cons[member])
        result.append(take_part(face_flux, 1, interior, along) - take_part(face_flux, 0, interior, along))
    return result

def residual(extended):
    states = primitive(extended)
    inner = [component[:, :, 2:-2, :] for component in states]
    circum = divergence(states, 2, 1)
    axial = divergence([jnp.pad(component, ((0, 0), (2, 2), (0, 0), (0, 0)), mode='edge') for component in inner], 1, 0)
    radial = divergence([jnp.pad(component, ((0, 0), (0, 0), (0, 0), (2, 2)), mode='edge') for component in inner], 3, 2)
    return jnp.stack([axial[member] + circum[member] + radial[member] for member in range(5)], axis=1)

def wrap_pad(field):
    return jnp.pad(field, ((0, 0), (0, 0), (0, 0), (2, 2), (0, 0)), mode='wrap')

def two_sweeps(single):
    field = single[None]
    first_sweep = residual(wrap_pad(field))
    segmented = field - segment_step * first_sweep
    return residual(wrap_pad(segmented))[0]

def transform_tables(instances):
    indices = jnp.arange(instances, dtype=jnp.int32)
    harmonic = jnp.where(indices < 2, indices * (instances // 2), indices // 2)
    phases = harmonic[:, None] * indices[None, :] % instances
    angles = phases.astype(jnp.float32) * (2.0 * math.pi / instances)
    sine_rows = (indices % 2 == 1) & (indices >= 2)
    basis = jnp.where(sine_rows[:, None], jnp.sin(angles), jnp.cos(angles))
    weights = jnp.where(indices < 2, 1.0 / instances, 2.0 / instances).astype(jnp.float32)
    return (basis * weights[:, None], basis.T)

def pair_solve(right, frequency):
    cosine_part = right[:, 0]
    sine_part = right[:, 1]
    determinant = diagonal_weight * diagonal_weight + frequency * frequency
    return jnp.stack([(diagonal_weight * cosine_part - frequency * sine_part) / determinant, (diagonal_weight * sine_part + frequency * cosine_part) / determinant], axis=1)

def neighbours(correction):
    circum = jnp.roll(correction, 1, 4) + jnp.roll(correction, -1, 4)
    padded = jnp.pad(correction, ((0, 0), (0, 0), (0, 0), (0, 0), (0, 0), (1, 1)))
    return circum + (padded[:, :, :, :, :, :-2] + padded[:, :, :, :, :, 2:])

def reference(state, multiples):
    second_sweep = lax.map(two_sweeps, state)
    forward, inverse = transform_tables(NT)
    residual_hat = jnp.dot(forward, second_sweep.reshape(NT, -1), precision=lax.Precision.HIGHEST)
    state_hat = jnp.dot(forward, state.reshape(NT, -1), precision=lax.Precision.HIGHEST)
    layout = (NT // 2, 2) + state.shape[1:]
    residual_hat = residual_hat.reshape(layout)
    state_hat = state_hat.reshape(layout)
    frequency = jnp.concatenate([jnp.zeros((1,), jnp.float32), base_rate * multiples.astype(jnp.float32)]).reshape(NT // 2, 1, 1, 1, 1)
    source = jnp.stack([frequency * state_hat[:, 1], -frequency * state_hat[:, 0]], axis=1)
    right_hand = -(residual_hat + source)
    correction = pair_solve(right_hand, frequency)
    for repeat in range(3):
        correction = pair_solve(right_hand + smooth_weight * neighbours(correction), frequency)
    change = jnp.dot(inverse, correction.reshape(NT, -1), precision=lax.Precision.HIGHEST)
    return change.reshape(state.shape)
```

```python
import math
from functools import partial

import jax
import jax.numpy as jnp
from jax import lax
from jax.experimental import pallas as pl
from jax.experimental.pallas import tpu as pltpu
from jax.sharding import PartitionSpec as P


heat_ratio = 1.4
segment_step = 0.05
smooth_weight = 0.5
base_rate = 0.5
diagonal_weight = 3.0
sweeps = 3
SUB, LANE = 8, 128


def minmod(a, b):
    return jnp.maximum(jnp.minimum(a, b), jnp.minimum(0.0, jnp.maximum(a, b)))


def primitive(q):
    inverse = 1.0 / q[0]
    u, v, w = q[1] * inverse, q[2] * inverse, q[3] * inverse
    kinetic = 0.5 * (q[1] * u + q[2] * v + q[3] * w)
    return [q[0], u, v, w, (heat_ratio - 1.0) * (q[4] - kinetic)]


def physical(s, normal):
    rho, p = s[0], s[4]
    vel = s[1:4]
    mom = [rho * c for c in vel]
    energy = p * (1.0 / (heat_ratio - 1.0)) + 0.5 * (mom[0] * vel[0] + mom[1] * vel[1] + mom[2] * vel[2])
    un, m = vel[normal], mom[normal]
    flux = [m]
    for i in range(3):
        f = m * vel[i]
        flux.append(f + p if i == normal else f)
    flux.append((energy + p) * un)
    gp = heat_ratio * p
    speed = jnp.abs(un) + gp * lax.rsqrt(gp * rho)
    return flux, [rho] + mom + [energy], speed


def face(left, right):
    fl, ql, al = left
    fr, qr, ar = right
    a = jnp.maximum(al, ar)
    return [(fl[i] + fr[i]) - a * (qr[i] - ql[i]) for i in range(5)]


class Shift:
    def __init__(self, axis):
        self.axis = axis
        self.size = (SUB, LANE)[axis]
        pos = lax.broadcasted_iota(jnp.int32, (SUB, LANE), axis)
        self.first = pos == 0
        self.last = pos == self.size - 1

    def down(self, pieces):
        rolled = [pltpu.roll(a, 1, self.axis) for a in pieces]
        edge = [pieces[0]] + rolled[:-1]
        return [jnp.where(self.first, e, r) for e, r in zip(edge, rolled)]

    def up(self, pieces, end=None):
        rolled = [pltpu.roll(a, self.size - 1, self.axis) for a in pieces]
        edge = rolled[1:] + [pieces[-1] if end is None else end]
        return [jnp.where(self.last, e, r) for e, r in zip(edge, rolled)]


def line_divergence(W, shift, normal):
    count = len(W[0])
    plus, minus = [], []
    for v in range(5):
        ahead = shift.up(W[v])
        d = [0.5 * (a - w) for a, w in zip(ahead, W[v])]
        rolled = [pltpu.roll(x, 1, shift.axis) for x in d]
        edge = [jnp.zeros_like(d[0])] + rolled[:-1]
        back = [jnp.where(shift.first, e, r) for e, r in zip(edge, rolled)]
        s = [minmod(x, y) for x, y in zip(back, d)]
        plus.append(shift.down([w + x for w, x in zip(W[v], s)]))
        minus.append([w - x for w, x in zip(W[v], s)])
    low, ends = [], None
    for i in range(count):
        left = physical([plus[v][i] for v in range(5)], normal)
        right = physical([minus[v][i] for v in range(5)], normal)
        low.append(face(left, right))
        ends = right[0]
    out = []
    for v in range(5):
        mine = [low[i][v] for i in range(count)]
        nxt = shift.up(mine, end=ends[v] + ends[v])
        out.append([b - a for a, b in zip(mine, nxt)])
    return out


def tiles(X, Z):
    return [(t, h) for t in range(X // SUB) for h in range(Z // LANE)]


def at(t, h):
    return pl.ds(t * SUB, SUB), pl.ds(h * LANE, LANE)


def xz_kernel(first, *refs):
    if first:
        src, prim, base, split = refs
    else:
        src, base = refs
        prim = src
    _, _, Y, X, Z = src.shape
    sx, sz = Shift(0), Shift(1)

    def row(y, carry):
        if first:
            for t, h in tiles(X, Z):
                r, c = at(t, h)
                q = [src[0, v, y, r, c] for v in range(5)]
                w = primitive(q)
                for v in range(5):
                    prim[0, v, y, r, c] = w[v]
        for h in range(Z // LANE):
            W = [[prim[0, v, y, at(t, h)[0], at(t, h)[1]] for t in range(X // SUB)] for v in range(5)]
            div = line_divergence(W, sx, 0)
            for t in range(X // SUB):
                r, c = at(t, h)
                for v in range(5):
                    base[0, v, y, r, c] = div[v][t]
        for t in range(X // SUB):
            W = [[prim[0, v, y, at(t, h)[0], at(t, h)[1]] for h in range(Z // LANE)] for v in range(5)]
            div = line_divergence(W, sz, 2)
            for h in range(Z // LANE):
                r, c = at(t, h)
                for v in range(5):
                    total = base[0, v, y, r, c] + div[v][h]
                    if first:
                        total = src[0, v, y, r, c] - (0.5 * segment_step) * total
                    base[0, v, y, r, c] = total
        return carry

    if first:
        spread(src, split)
    lax.fori_loop(0, Y, row, 0)


def spread(src, split):
    _, V, Y, X, _ = src.shape
    groups = split.shape[0]
    xl = X // groups
    per = max(1, SUB // xl)

    def rows(i, carry):
        for v in range(V):
            for g in range(groups):
                parts = [src[0, v, i * per + j, pl.ds(g * xl, xl), :] for j in range(per)]
                split[g, 0, v, pl.ds(pl.multiple_of(i * per * xl, SUB), per * xl), :] = jnp.concatenate(parts, axis=0)
        return carry

    lax.fori_loop(0, Y // per, rows, 0)


def y_kernel(first, *refs):
    prim, low, high, base, out = refs
    _, _, Y, X, Z = prim.shape

    for t, h in tiles(X, Z):
        r, c = at(t, h)

        def load(j):
            if j < 0:
                w = [low[0, v, 2 + j, r, c] for v in range(5)]
            elif j >= Y:
                w = [high[0, v, j - Y, r, c] for v in range(5)]
            else:
                return [prim[0, v, j, r, c] for v in range(5)]
            return primitive(w) if first else w

        here, ahead = load(-2), load(-1)
        d = [0.5 * (a - w) for a, w in zip(ahead, here)]
        left = before = None
        for j in range(-1, Y + 1):
            here, ahead = ahead, load(j + 1)
            back, d = d, [0.5 * (a - w) for a, w in zip(ahead, here)]
            s = [minmod(x, y) for x, y in zip(back, d)]
            if j >= 0:
                right = physical([w - x for w, x in zip(here, s)], 1)
                flux = face(left, right)
                if j >= 1:
                    total = [b - a for a, b in zip(before, flux)]
                    if first:
                        q = [base[0, v, j - 1, r, c] - (0.5 * segment_step) * total[v] for v in range(5)]
                        w = primitive(q)
                        for v in range(5):
                            out[0, v, j - 1, r, c] = w[v]
                    else:
                        groups = out.shape[0]
                        xl = X // groups
                        for v in range(5):
                            val = 0.5 * (base[0, v, j - 1, r, c] + total[v])
                            for part in range(SUB // xl):
                                g = t * (SUB // xl) + part
                                out[g, 0, v, pl.ds((j - 1) * xl, xl), c] = val[part * xl:(part + 1) * xl]
                before = flux
            if j < Y:
                left = physical([w + x for w, x in zip(here, s)], 1)


def combine(terms):
    total = None
    for coef, val in terms:
        if abs(coef) < 1e-9:
            continue
        neg = coef < 0
        term = val if abs(abs(coef) - 1.0) < 1e-9 else val * abs(coef)
        if total is None:
            total = -term if neg else term
        else:
            total = total - term if neg else total + term
    return total


def forward_sums(x):
    N = len(x)
    M, Q = N // 2, N // 4
    even = [None] + [x[n] + x[N - n] for n in range(1, M)]
    odd = [None] + [x[n] - x[N - n] for n in range(1, M)]
    ends = (x[0] + x[M], x[0] - x[M])
    es = [None] + [even[n] + even[M - n] for n in range(1, Q)]
    ed = [None] + [even[n] - even[M - n] for n in range(1, Q)]
    os = [None] + [odd[n] + odd[M - n] for n in range(1, Q)]
    od = [None] + [odd[n] - odd[M - n] for n in range(1, Q)]
    cosine, sine = [], [None]
    for h in range(M + 1):
        src = ed if h % 2 else es
        terms = [(1.0, ends[h % 2])] + [(math.cos(2 * math.pi * h * n / N), src[n]) for n in range(1, Q)]
        if h % 2 == 0:
            terms.append((math.cos(math.pi * h / 2), even[Q]))
        cosine.append(combine(terms))
    for h in range(1, M):
        src = os if h % 2 else od
        terms = [(math.sin(2 * math.pi * h * n / N), src[n]) for n in range(1, Q)]
        if h % 2:
            terms.append((math.sin(math.pi * h / 2), odd[Q]))
        sine.append(combine(terms))
    return cosine, sine


def inverse_sums(a, b):
    M = len(a)
    N, Q = 2 * M, M // 2
    x = [None] * N
    for n in range(Q + 1):
        c = lambda k: math.cos(2 * math.pi * k * n / N)
        s = lambda k: math.sin(2 * math.pi * k * n / N)
        ce = combine([(1.0, a[0]), (1.0 if n % 2 == 0 else -1.0, b[0])] + [(c(k), a[k]) for k in range(2, M, 2)])
        co = combine([(c(k), a[k]) for k in range(1, M, 2)])
        se = combine([(s(k), b[k]) for k in range(2, M, 2)])
        so = combine([(s(k), b[k]) for k in range(1, M, 2)])
        add = lambda p, q: p if q is None else (q if p is None else p + q)
        sub = lambda p, q: p if q is None else (-q if p is None else p - q)
        cp, cm = add(ce, co), sub(ce, co)
        sp, sm = add(so, se), sub(so, se)
        x[n] = add(cp, sp)
        if n > 0:
            x[N - n] = sub(cp, sp)
        if n != M - n:
            x[M - n] = add(cm, sm)
            if M - n < M:
                x[M + n] = sub(cm, sm)
    return x


def rhs_kernel(rates, res, st, out, low, high):
    N, _, rows, Z = res.shape
    K, _, Y, _, _ = out.shape
    xl = rows // Y
    halo = low.shape[2]
    per = max(1, SUB // xl)
    height = per * xl

    def put(k, y, half, val, c):
        place = pl.ds(half * xl, xl)
        out[k, 0, y, place, c] = val
        if y < halo:
            low[k, 0, y, place, c] = val
        if y >= Y - halo:
            high[k, 0, y - (Y - halo), place, c] = val

    for tile in range(rows // height):
        for h in range(Z // LANE):
            c = pl.ds(h * LANE, LANE)
            r = pl.ds(tile * height, height)
            rc, rs = forward_sums([res[n, 0, r, c] for n in range(N)])
            sc, ss = forward_sums([st[n, 0, r, c] for n in range(N)])
            for k in range(K):
                w = rates[k]
                if k == 0:
                    ra, rb, sa, sb, scale = rc[0], rc[K], sc[0], sc[K], -1.0 / N
                else:
                    ra, rb, sa, sb, scale = rc[k], rs[k], sc[k], ss[k], -2.0 / N
                a = scale * (ra + w * sb)
                b = scale * (rb - w * sa)
                for i in range(per):
                    y = tile * per + i
                    put(k, y, 0, a[i * xl:(i + 1) * xl], c)
                    put(k, y, 1, b[i * xl:(i + 1) * xl], c)


def smooth_kernel(rates, core, low, high, out, corr):
    K, _, Y, two, Z = core.shape
    xl = two // 2
    N = 2 * K
    halo = low.shape[2]
    nh = Z // LANE
    lane = lax.broadcasted_iota(jnp.int32, (two, LANE), 1)
    head, tail = lane == 0, lane == LANE - 1
    half = lax.broadcasted_iota(jnp.int32, (two, LANE), 0) < xl
    zero = jnp.zeros((two, LANE), jnp.float32)

    def pair(k, carry):
        w = rates[k]
        det = jnp.full((two, LANE), diagonal_weight * diagonal_weight, jnp.float32) + w * w
        inv = 1.0 / det
        straight = diagonal_weight * inv
        cross = jnp.where(half, -w, w) * inv

        def solve(v):
            other = jnp.concatenate([v[xl:], v[:xl]], axis=0)
            return straight * v + cross * other

        def load(y, h):
            c = pl.ds(h * LANE, LANE)
            if y < 0:
                return low[k, 0, halo + y, :, c]
            if y >= Y:
                return high[k, 0, y - Y, :, c]
            return core[k, 0, y, :, c]

        first = {y: [solve(load(y, h)) for h in range(nh)] for y in range(-halo, Y + halo)}
        cur = first
        for it in range(1, sweeps + 1):
            nxt = {}
            for y in range(-halo + it, Y + halo - it):
                mid = cur[y]
                right = [pltpu.roll(m, LANE - 1, 1) for m in mid]
                left = [pltpu.roll(m, 1, 1) for m in mid]
                row = []
                for h in range(nh):
                    fwd = jnp.where(tail, right[h + 1] if h + 1 < nh else zero, right[h])
                    bwd = jnp.where(head, left[h - 1] if h > 0 else zero, left[h])
                    nb = (cur[y - 1][h] + cur[y + 1][h]) + (fwd + bwd)
                    row.append(first[y][h] + solve(smooth_weight * nb))
                nxt[y] = row
            cur = nxt
        for y in range(Y):
            for h in range(nh):
                corr[k, h, pl.ds(y * two, two), :] = cur[y][h]
        return carry

    lax.fori_loop(0, K, pair, 0)
    for x in range(xl):
        for h in range(nh):
            c = pl.ds(h * LANE, LANE)
            a = [corr[k, h, pl.ds(x, Y, stride=two), :] for k in range(K)]
            b = [corr[k, h, pl.ds(xl + x, Y, stride=two), :] for k in range(K)]
            vals = inverse_sums(a, b)
            for n in range(N):
                out[n, 0, x, :, c] = vals[n]


def struct(*shape):
    return jax.ShapeDtypeStruct(shape, jnp.float32)


def params():
    return pltpu.CompilerParams(dimension_semantics=("arbitrary",))


def by_instance(*shape):
    return pl.BlockSpec((1,) + shape, lambda n: (n,) + (0,) * len(shape))


def second(*shape):
    return pl.BlockSpec((shape[0], 1) + shape[1:], lambda n: (0, n) + (0,) * (len(shape) - 1))


def cost(points, flops, arrays):
    return pl.CostEstimate(flops=points * flops, bytes_accessed=points * 4 * arrays, transcendentals=0)


def xz_call(src, first, groups):
    n, V, Y, X, Z = src.shape
    xl = X // groups
    field = by_instance(V, Y, X, Z)
    outs, specs = [src.shape], [field]
    if first:
        outs = [src.shape, src.shape, (groups, n, V, Y * xl, Z)]
        specs = [field, field, second(groups, V, Y * xl, Z)]
    return pl.pallas_call(
        partial(xz_kernel, first),
        grid=(n,),
        in_specs=[field],
        out_specs=specs,
        out_shape=[struct(*s) for s in outs],
        compiler_params=params(),
        cost_estimate=cost(n * Y * X * Z, 400, 4 * V),
        name="sweep_xz_first" if first else "sweep_xz_second",
    )(src)


def y_call(prim, low, high, base, first, groups):
    n, V, Y, X, Z = prim.shape
    xl = X // groups
    field = by_instance(V, Y, X, Z)
    edge = by_instance(V, 2, X, Z)
    return pl.pallas_call(
        partial(y_kernel, first),
        grid=(n,),
        in_specs=[field, edge, edge, field],
        out_specs=field if first else second(groups, V, Y * xl, Z),
        out_shape=struct(*prim.shape) if first else struct(groups, n, V, Y * xl, Z),
        compiler_params=params(),
        cost_estimate=cost(n * Y * X * Z, 200, 3 * V),
        name="sweep_y_first" if first else "sweep_y_second",
    )(prim, low, high, base)


def rhs_call(rates, res, st, Y):
    N, V, rows, Z = res.shape
    K, xl = N // 2, rows // Y
    field = second(N, rows, Z)
    smem = pl.BlockSpec(memory_space=pltpu.SMEM)
    return pl.pallas_call(
        rhs_kernel,
        grid=(V,),
        in_specs=[smem, field, field],
        out_specs=[second(K, Y, 2 * xl, Z), second(K, sweeps, 2 * xl, Z), second(K, sweeps, 2 * xl, Z)],
        out_shape=[struct(K, V, Y, 2 * xl, Z), struct(K, V, sweeps, 2 * xl, Z), struct(K, V, sweeps, 2 * xl, Z)],
        compiler_params=params(),
        cost_estimate=cost(N * V * rows * Z, 20, 3),
        name="right_hand",
    )(rates, res, st)


def smooth_call(rates, core, low, high):
    K, V, Y, two, Z = core.shape
    xl = two // 2
    smem = pl.BlockSpec(memory_space=pltpu.SMEM)
    edge = second(K, sweeps, two, Z)
    return pl.pallas_call(
        smooth_kernel,
        grid=(V,),
        in_specs=[smem, second(K, Y, two, Z), edge, edge],
        out_specs=second(2 * K, xl, Y, Z),
        out_shape=struct(2 * K, V, xl, Y, Z),
        scratch_shapes=[pltpu.VMEM((K, Z // LANE, Y * two, LANE), jnp.float32)],
        compiler_params=params(),
        cost_estimate=cost(2 * K * V * xl * Y * Z, 60, 3),
        name="smooth",
    )(rates, core, low, high)


def halos(head, tail):
    count = lax.axis_size("blk")
    low = lax.ppermute(tail, "blk", [(i, (i + 1) % count) for i in range(count)])
    high = lax.ppermute(head, "blk", [((i + 1) % count, i) for i in range(count)])
    return low, high


def exchange(x):
    return lax.all_to_all(x, "inst", split_axis=0, concat_axis=0, tiled=True)


def body(state, multiples):
    groups = lax.axis_size("inst")
    n, V, X, Y, Z = state.shape
    N, xl = n * groups, X // groups
    rates = jnp.concatenate([jnp.zeros((1,), jnp.float32), base_rate * multiples.astype(jnp.float32)])

    turn = lambda a: jnp.transpose(a, (0, 1, 3, 2, 4))
    own, head, tail = lax.optimization_barrier((state, turn(state[:, :, :, :2]), turn(state[:, :, :, Y - 2:])))
    low, high = halos(head, tail)
    prim, base, split = xz_call(turn(own), True, groups)
    prim2 = y_call(prim, low, high, base, True, groups)

    low, high = halos(prim2[:, :, :2], prim2[:, :, Y - 2:])
    st = exchange(split).reshape(N, V, Y * xl, Z)
    (base2,) = xz_call(prim2, False, groups)
    second_sweep = y_call(prim2, low, high, base2, False, groups)
    res = exchange(second_sweep).reshape(N, V, Y * xl, Z)

    core, head, tail = rhs_call(rates, res, st, Y)
    low, high = halos(head, tail)
    change = smooth_call(rates, core, low, high)
    back = exchange(change.reshape(groups, n, V, xl, Y, Z))
    return jnp.transpose(back, (1, 2, 0, 3, 4, 5)).reshape(state.shape)


def solution(mesh):
    return jax.shard_map(
        body,
        mesh=mesh,
        in_specs=(P("inst", None, None, "blk", None), P()),
        out_specs=P("inst", None, None, "blk", None),
        check_vma=False,
    )
```
